32 devices in a mesh: row: 8 (over y, x, core), gz: 4 (over z).
Axes of the slice: x: 2, y: 2, z: 4, core: 2. Of those that a mesh axis runs over, the one named last changes fastest.
Arguments:
- velocity_x: bfloat16 [2, 8, 1024, 1024], P(None, None, 'row', 'gz'), may hold values from -6 to 6
- velocity_y: bfloat16 [2, 8, 1024, 1024], P(None, None, 'row', 'gz'), may hold values from -6 to 6
- velocity_z: bfloat16 [2, 8, 1024, 1024], P(None, None, 'row', 'gz'), may hold values from -6 to 6
- spacing: float32 [64], replicated, may hold values from 0.5 to 2
- level_index: int32 [1024], replicated, may hold values from 0 to 63
- plane_index: int32 [8], replicated, may hold values from 4 to 128
Outputs:
- pressure: float32 [2, 8, 1024, 1024], P(None, None, 'row', 'gz')
The draws below stay inside these ranges and needn't reach their ends.
All inputs are finite; a program needn't handle non-finite values.
Results may differ from the reference program's by a relative error of at most 0.002.
The reference program's roundings to bfloat16 on the way count: a program that leaves them out, or rounds other values in their place, can miss the bound.
Values may be sent and summed in bfloat16 or wider, within the bound.
A program may use at most 64 MiB of HBM per device.

```python
import math
import jax
import jax.numpy as jnp
from jax import lax

NX = 1024
NZ = 1024
NLEV = 64
P_SIZE = 8


def plant(values, rng, low, largest):
    dims = values.shape
    spot = [jax.random.randint(jax.random.fold_in(rng, axis), (), 0, dims[axis]) for axis in range(len(dims))]
    values = values.at[tuple(spot)].set(low)
    longest = dims.index(max(dims))
    spot[longest] = (spot[longest] + 1) % dims[longest]
    return values.at[tuple(spot)].set(largest)


def shard_levels(own_key, shape, cuts, low, high):
    factor_of, own = 1.0, jax.random.fold_in(own_key, 6)
    for position, shards_of in cuts:
        heights = jnp.exp(jax.random.uniform(jax.random.fold_in(own, position), (shards_of,), jnp.float32, low / len(cuts), high / len(cuts)))
        factor_of = factor_of * jnp.repeat(heights, shape[position] // shards_of).reshape([-1 if axis == position else 1 for axis in range(len(shape))])
    return factor_of


def centred(key, dims, deviation, limit, split=(), kind=jnp.bfloat16):
    level = shard_levels(key, dims, split, -0.22, 0.18) if split else 1.0
    array = jax.random.normal(key, dims, jnp.float32) * deviation * level
    return jnp.minimum(jnp.maximum(array, -limit), limit).astype(kind)


def setup_inputs(seed: int = 0) -> dict:
    key_of = jax.random.split(jax.random.key(seed), 7)
    velocity_x = centred(key_of[0], (2, P_SIZE, NX, NZ), 1.0, 6.0, ((2, 8), (3, 4)))
    velocity_y = centred(key_of[1], (2, P_SIZE, NX, NZ), 1.0, 6.0, ((2, 8), (3, 4)))
    velocity_z = centred(key_of[2], (2, P_SIZE, NX, NZ), 1.0, 6.0, ((2, 8), (3, 4)))
    spacing = jnp.clip(jnp.exp(jax.random.uniform(key_of[3], (NLEV,), jnp.float32, math.log(0.5), math.log(2.0))), 0.5, 2.0)
    level_index = plant(jax.random.randint(key_of[4], (NZ,), 0, NLEV), jax.random.fold_in(key_of[4], 1), 0, NLEV - 1).astype(jnp.int32)
    plane_index = plant(jax.random.randint(key_of[5], (P_SIZE,), 4, 129), jax.random.fold_in(key_of[5], 1), 4, 128).astype(jnp.int32)
    return {"velocity_x": velocity_x, "velocity_y": velocity_y, "velocity_z": velocity_z, "spacing": spacing, "level_index": level_index, "plane_index": plane_index}


full_turn = 2.0 * math.pi
wave_unit = 2.0 * math.pi / 2048.0


def band_coefficients(cell_width):
    length = cell_width.shape[0]
    index = jnp.arange(length, dtype=jnp.int32)
    previous = jnp.concatenate([cell_width[:1], cell_width[:-1]])
    following = jnp.concatenate([cell_width[1:], cell_width[-1:]])
    lower_band = jnp.where(index > 0, 1.0 / (0.5 * (previous + cell_width) * cell_width), 0.0)
    upper_band = jnp.where(index < length - 1, 1.0 / (0.5 * (cell_width + following) * cell_width), 0.0)
    return lower_band, upper_band


def thomas(lower_band, diagonal, upper_band, right_real, right_imag):
    rows = (lower_band, upper_band, diagonal.T, right_real.T, right_imag.T)

    def sweep(carry, row):
        ratio_prev, real_prev, imag_prev = carry
        low_coef, up_coef, diag_col, real_in, imag_in = row
        pivot = diag_col - low_coef * ratio_prev
        ratio = up_coef / pivot
        real_now = (real_in - low_coef * real_prev) / pivot
        imag_now = (imag_in - low_coef * imag_prev) / pivot
        return (ratio, real_now, imag_now), (ratio, real_now, imag_now)

    zeros = jnp.zeros((diagonal.shape[0],), diagonal.dtype)
    unused, (ratios, reals, imags) = lax.scan(sweep, (zeros, zeros, zeros), rows)

    def back(carry, row):
        next_real, next_imag = carry
        ratio, real_now, imag_now = row
        value_real = real_now - ratio * next_real
        value_imag = imag_now - ratio * next_imag
        return (value_real, value_imag), (value_real, value_imag)

    unused, (sol_real, sol_imag) = lax.scan(back, (zeros, zeros), (ratios, reals, imags), reverse=True)
    return sol_real.T, sol_imag.T


def reference(velocity_x, velocity_y, velocity_z, spacing, level_index, plane_index):
    cell_width = spacing[level_index]
    lower_band, upper_band = band_coefficients(cell_width)
    modes = jnp.arange(NX, dtype=jnp.int32)
    signed = jnp.where(modes >= NX // 2, modes - NX, modes)
    wave_x = signed.astype(jnp.float32) * (full_turn / NX)

    def one_plane(item):
        along, across, upward, index_y = item
        wave_y = index_y.astype(jnp.float32) * wave_unit
        up_real = upward[0].astype(jnp.float32)
        up_imag = upward[1].astype(jnp.float32)
        zero_col = jnp.zeros((NX, 1), jnp.float32)
        below_real = jnp.concatenate([zero_col, up_real[:, :-1]], axis=1)
        below_imag = jnp.concatenate([zero_col, up_imag[:, :-1]], axis=1)
        across_real = across[0].astype(jnp.float32)
        across_imag = across[1].astype(jnp.float32)
        source_real = (-wave_y * across_imag + (up_real - below_real) / cell_width).astype(jnp.bfloat16)
        source_imag = (wave_y * across_real + (up_imag - below_imag) / cell_width).astype(jnp.bfloat16)
        source_real, source_imag = lax.optimization_barrier((source_real, source_imag))
        source_hat = jnp.fft.fft(source_real.astype(jnp.float32) + 1j * source_imag.astype(jnp.float32), axis=0)
        along_hat = jnp.fft.fft(along[0].astype(jnp.float32) + 1j * along[1].astype(jnp.float32), axis=0)
        right_hat = source_hat + 1j * wave_x[:, None] * along_hat
        wave_sq = wave_x * wave_x + wave_y * wave_y
        diagonal = -(lower_band + upper_band)[None, :] - wave_sq[:, None]
        sol_real, sol_imag = thomas(lower_band, diagonal, upper_band, jnp.real(right_hat), jnp.imag(right_hat))
        field = jnp.fft.ifft(sol_real + 1j * sol_imag, axis=0)
        return jnp.stack([jnp.real(field), jnp.imag(field)]).astype(jnp.float32)

    stacked = lax.map(one_plane, (jnp.moveaxis(velocity_x, 1, 0), jnp.moveaxis(velocity_y, 1, 0), jnp.moveaxis(velocity_z, 1, 0), plane_index))
    return jnp.moveaxis(stacked, 0, 1)
```

```python
import functools
import math

import jax
import jax.numpy as jnp
import numpy as np
from jax import lax
from jax.experimental import pallas as pl
from jax.experimental.pallas import tpu as pltpu
from jax.sharding import PartitionSpec as P

RADIX = 8
LANES = 128

full_turn = 2.0 * math.pi
wave_unit = 2.0 * math.pi / 2048.0


def phase_tables(total_x):
    inner = total_x // RADIX
    k1 = np.arange(RADIX)[:, None, None]
    m = np.arange(inner)[None, :, None]
    k2 = np.arange(inner)[None, None, :]
    angle = -full_turn * ((m * (k1 + RADIX * k2)) % total_x) / total_x
    cos, sin = np.cos(angle), np.sin(angle)
    table = np.concatenate(
        [np.concatenate([cos, sin], axis=2), np.concatenate([-sin, cos], axis=2)], axis=1
    )
    high = table.astype(jnp.bfloat16)
    low = (table - high.astype(np.float64)).astype(jnp.bfloat16)
    return high, low


def radix_eight(re, im, sign):
    half = math.sqrt(0.5)
    add = lambda a, b: (a[0] + b[0], a[1] + b[1])
    sub = lambda a, b: (a[0] - b[0], a[1] - b[1])
    turn = lambda a: (-sign * a[1], sign * a[0])
    x = list(zip(re, im))
    even = [add(x[j], x[j + 4]) for j in range(4)]
    odd = [sub(x[j], x[j + 4]) for j in range(4)]
    a, b = odd[1]
    odd[1] = (half * (a - sign * b), half * (b + sign * a))
    odd[2] = turn(odd[2])
    a, b = odd[3]
    odd[3] = (half * (-a - sign * b), half * (sign * a - b))

    def four(v):
        t0, t1 = add(v[0], v[2]), sub(v[0], v[2])
        t2, t3 = add(v[1], v[3]), turn(sub(v[1], v[3]))
        return [add(t0, t2), add(t1, t3), sub(t0, t2), sub(t1, t3)]

    e, o = four(even), four(odd)
    out = [e[0], o[0], e[1], o[1], e[2], o[2], e[3], o[3]]
    return [v[0] for v in out], [v[1] for v in out]


def split(value):
    high = value.astype(jnp.bfloat16)
    return high, (value - high.astype(jnp.float32)).astype(jnp.bfloat16)


def kernel(
    rows, groups,
    vx, vy_hbm, vz_hbm, wh_hbm, wl_hbm, level_row, spacing, level, plane,
    out,
    vy, vz, wh, wl, wall_out, wall_in, src, got_u, got_s,
    yh, yl, rhs_re, rhs_im, qq, lq, uq, from_lo, from_hi, coef, edge, solved, spec, back,
    load_sem, own_sem, u_send, u_recv, s_send, s_recv, w_send, w_recv,
    c_send, c_recv, e_send, e_recv, p_send, p_recv,
):
    me = lax.axis_index("row")
    gz = lax.axis_index("gz")
    planes, part, depth = vx.shape[1:]
    total_x = part * rows
    inner = total_x // RADIX
    total_z = level.shape[0]
    levels = spacing.shape[0]
    f32 = jnp.float32

    loads = [
        pltpu.make_async_copy(vz_hbm, vz, load_sem.at[0]),
        pltpu.make_async_copy(vy_hbm, vy, load_sem.at[1]),
        pltpu.make_async_copy(wh_hbm, wh, load_sem.at[2]),
        pltpu.make_async_copy(wl_hbm, wl, load_sem.at[3]),
    ]
    for load in loads:
        load.start()
    mine = pl.ds(pl.multiple_of(me * part, part), part)
    own_u = pltpu.make_async_copy(vx.at[:, me], got_u.at[:, mine, :], own_sem.at[0])
    own_u.start()

    barrier = pltpu.get_barrier_semaphore()
    for i in range(1, rows):
        pl.semaphore_signal(
            barrier, inc=1, device_id={"row": lax.rem(me + i, rows)},
            device_id_type=pl.DeviceIdType.MESH,
        )
    for i in range(1, groups):
        pl.semaphore_signal(
            barrier, inc=1, device_id={"gz": lax.rem(gz + i, groups)},
            device_id_type=pl.DeviceIdType.MESH,
        )
    pl.semaphore_wait(barrier, rows + groups - 2)

    def to_row(source, target, send, recv, i):
        return pltpu.make_async_remote_copy(
            src_ref=source, dst_ref=target, send_sem=send, recv_sem=recv,
            device_id={"row": lax.rem(me + i, rows)}, device_id_type=pl.DeviceIdType.MESH,
        )

    def to_group(source, target, send, recv, i):
        return pltpu.make_async_remote_copy(
            src_ref=source, dst_ref=target, send_sem=send, recv_sem=recv,
            device_id={"gz": lax.rem(gz + i, groups)}, device_id_type=pl.DeviceIdType.MESH,
        )

    sends_u = []
    for i in range(1, rows):
        copy = to_row(
            vx.at[:, lax.rem(me + i, rows)], got_u.at[:, mine, :], u_send.at[i], u_recv.at[i], i
        )
        copy.start()
        sends_u.append(copy)

    lane_small = lax.broadcasted_iota(jnp.int32, (part, LANES), 1)
    loads[0].wait()
    packed = jnp.zeros((part, LANES), f32)
    for c in range(2):
        for p in range(planes):
            slot = c * planes + p
            tile = vz[c, p, :, depth - LANES :].astype(f32)
            packed = jnp.where(lane_small == slot, pltpu.roll(tile, (slot + 1) % LANES, 1), packed)
    wall_out[...] = packed.astype(jnp.bfloat16)
    wall_copy = to_group(wall_out, wall_in, w_send, w_recv, 1)

    @pl.when(gz < groups - 1)
    def _():
        wall_copy.start()

    base = gz * depth
    own_level = level_row[:, pl.ds(pl.multiple_of(base, LANES), depth)]
    width = jnp.zeros((1, depth), f32)
    for n in range(levels):
        width = jnp.where(own_level == n, spacing[n], width)
    loads[1].wait()

    @pl.when(gz > 0)
    def _():
        wall_copy.wait_recv()

    @pl.when(gz == 0)
    def _():
        wall_in[...] = jnp.zeros_like(wall_in)

    first_lane = lax.broadcasted_iota(jnp.int32, (part, depth), 1) == 0

    def slope_of(c, p):
        values = vz[c, p].astype(f32)
        slot = c * planes + p
        turned = pltpu.roll(wall_in[...].astype(f32), lax.rem(LANES - slot, LANES), 1)
        if depth > LANES:
            turned = jnp.concatenate([turned] * (depth // LANES), axis=1)
        below = jnp.where(first_lane, turned, pltpu.roll(values, 1, 1))
        return (values - below) / width

    def make_source(i, carry):
        p = lax.rem(me + i, rows)
        wave = jnp.full((1, depth), plane[p], jnp.int32).astype(f32) * wave_unit
        src[p, 0] = (-wave * vy[1, p].astype(f32) + slope_of(0, p)).astype(jnp.bfloat16)
        src[p, 1] = (wave * vy[0, p].astype(f32) + slope_of(1, p)).astype(jnp.bfloat16)

        @pl.when(i > 0)
        def _():
            to_row(src.at[p], got_s.at[:, mine, :], s_send.at[i], s_recv.at[i], i).start()

        return carry

    lax.fori_loop(1, rows, make_source, 0)
    make_source(0, 0)
    own_s = pltpu.make_async_copy(src.at[me], got_s.at[:, mine, :], own_sem.at[1])
    own_s.start()

    tile = (RADIX, inner)
    k1s = lax.broadcasted_iota(jnp.int32, tile, 0)
    k2s = lax.broadcasted_iota(jnp.int32, tile, 1)
    modes = k1s + RADIX * k2s
    wave_x = jnp.where(modes >= total_x // 2, modes - total_x, modes).astype(f32) * (
        full_turn / total_x
    )
    wave_y = jnp.full(tile, plane[me], jnp.int32).astype(f32) * wave_unit
    wave_sq = wave_x * wave_x + wave_y * wave_y

    def width_at(j):
        return jnp.full(tile, spacing[level[jnp.clip(j, 0, total_z - 1)]], f32)

    def factor(j, carry):
        excess, h_prev, h_now, homog = carry
        at = base + j
        h_next = width_at(at + 1)
        flag_lo = jnp.where(at > 0, 1.0, 0.0).astype(f32)
        flag_hi = jnp.where(at < total_z - 1, 1.0, 0.0).astype(f32)
        lower = flag_lo / (0.5 * (h_prev + h_now) * h_now)
        upper = flag_hi / (0.5 * (h_now + h_next) * h_now)
        s = wave_sq + lower * excess
        q = 1.0 / (upper + s)
        homog = lower * q * homog
        rows_j = pl.ds(pl.multiple_of(j * RADIX, RADIX), RADIX)
        qq[rows_j, :] = q
        lq[rows_j, :] = lower * q
        uq[rows_j, :] = upper * q
        from_lo[rows_j, :] = homog
        return s * q, h_now, h_next, homog

    one = jnp.ones(tile, f32)
    lax.fori_loop(0, depth, factor, (one, width_at(base - 1), width_at(base), one))

    def factor_back(t, carry):
        lo, hi = carry
        j = depth - 1 - t
        rows_j = pl.ds(pl.multiple_of(j * RADIX, RADIX), RADIX)
        ratio = uq[rows_j, :]
        lo = from_lo[rows_j, :] + ratio * lo
        hi = ratio * hi
        from_lo[rows_j, :] = lo
        from_hi[rows_j, :] = hi
        return lo, hi

    lax.fori_loop(0, depth, factor_back, (jnp.zeros(tile, f32), one))
    top = (depth - 1) * RADIX
    coef[gz, 0] = from_lo[0:RADIX, :]
    coef[gz, 1] = from_hi[0:RADIX, :]
    coef[gz, 2] = from_lo[top : top + RADIX, :]
    coef[gz, 3] = from_hi[top : top + RADIX, :]
    sends_c = []
    for i in range(1, groups):
        copy = to_group(coef.at[gz], coef.at[gz], c_send.at[i], c_recv.at[i], i)
        copy.start()
        sends_c.append(copy)

    step = 16

    def first_stage(field):
        def body(t, carry):
            at = pl.multiple_of(t * step, step)
            for lane in range(0, depth, LANES):
                cols = pl.ds(lane, LANES)
                re = [field[0, pl.ds(r * inner + at, step), cols].astype(f32) for r in range(RADIX)]
                im = [field[1, pl.ds(r * inner + at, step), cols].astype(f32) for r in range(RADIX)]
                re, im = radix_eight(re, im, -1.0)
                for k in range(RADIX):
                    h, l = split(re[k])
                    yh[k, pl.ds(at, step), cols] = h
                    yl[k, pl.ds(at, step), cols] = l
                    h, l = split(im[k])
                    yh[k, pl.ds(inner + at, step), cols] = h
                    yl[k, pl.ds(inner + at, step), cols] = l
            return carry

        lax.fori_loop(0, inner // step, body, 0)

    over_rows = (((0,), (0,)), ((), ()))
    over_last = (((1,), (1,)), ((), ()))

    def dot(a, b, dims):
        return lax.dot_general(a, b, dims, preferred_element_type=f32)

    def second_stage(combine):
        def body(k, carry):
            h, l, a, b = yh[k], yl[k], wh[k], wl[k]
            hat = dot(h, a, over_rows) + dot(h, b, over_rows) + dot(l, a, over_rows)
            combine(k, hat[:, :inner], hat[:, inner:])
            return carry

        lax.fori_loop(0, RADIX, body, 0)

    def put_along(k, re, im):
        number = k + RADIX * lax.broadcasted_iota(jnp.int32, (1, inner), 1)
        column = jnp.where(number >= total_x // 2, number - total_x, number).astype(f32) * (
            full_turn / total_x
        )
        where = pl.ds(k, depth, stride=RADIX)
        rhs_re[where, :] = -column * im
        rhs_im[where, :] = column * re

    def put_source(k, re, im):
        where = pl.ds(k, depth, stride=RADIX)
        rhs_re[where, :] = rhs_re[where, :] + re
        rhs_im[where, :] = rhs_im[where, :] + im

    own_u.wait()
    for copy in sends_u:
        copy.wait()
    for load in loads[2:]:
        load.wait()
    first_stage(got_u)
    second_stage(put_along)
    own_s.wait()
    for i in range(1, rows):
        to_row(
            src.at[lax.rem(me + i, rows)], got_s.at[:, mine, :], s_send.at[i], s_recv.at[i], i
        ).wait()
    first_stage(got_s)
    second_stage(put_source)

    def sweep(j, carry):
        re, im = carry
        rows_j = pl.ds(pl.multiple_of(j * RADIX, RADIX), RADIX)
        q, low = qq[rows_j, :], lq[rows_j, :]
        re = low * re - q * rhs_re[rows_j, :]
        im = low * im - q * rhs_im[rows_j, :]
        rhs_re[rows_j, :] = re
        rhs_im[rows_j, :] = im
        return re, im

    def sweep_back(t, carry):
        re, im = carry
        rows_j = pl.ds(pl.multiple_of((depth - 1 - t) * RADIX, RADIX), RADIX)
        ratio = uq[rows_j, :]
        re = rhs_re[rows_j, :] + ratio * re
        im = rhs_im[rows_j, :] + ratio * im
        rhs_re[rows_j, :] = re
        rhs_im[rows_j, :] = im
        return re, im

    zero = jnp.zeros(tile, f32)
    lax.fori_loop(0, depth, sweep, (zero, zero), unroll=4)
    lax.fori_loop(0, depth, sweep_back, (zero, zero), unroll=4)

    edge[gz, 0] = rhs_re[0:RADIX, :]
    edge[gz, 1] = rhs_re[top : top + RADIX, :]
    edge[gz, 2] = rhs_im[0:RADIX, :]
    edge[gz, 3] = rhs_im[top : top + RADIX, :]
    sends_e = []
    for i in range(1, groups):
        copy = to_group(edge.at[gz], edge.at[gz], e_send.at[i], e_recv.at[i], i)
        copy.start()
        sends_e.append(copy)
    for copy in sends_c:
        copy.wait()
    for copy in sends_e:
        copy.wait()
    if groups > 1 or True:
        last_const, last_ratio = [(zero, zero)], [zero]
        head_const, head_ratio = [], []
        for b in range(groups):
            a0, b0, a1, b1 = (coef[b, n] for n in range(4))
            inv = 1.0 / (1.0 - a0 * last_ratio[b])
            ratio = b0 * inv
            head_ratio.append(ratio)
            heads, lasts = [], []
            for part_of in range(2):
                prev = last_const[b][part_of]
                head = (edge[b, 2 * part_of] + a0 * prev) * inv
                heads.append(head)
                lasts.append(edge[b, 2 * part_of + 1] + a1 * (prev + last_ratio[b] * head))
            head_const.append(heads)
            last_const.append(lasts)
            last_ratio.append(a1 * last_ratio[b] * ratio + b1)
        for part_of in range(2):
            following = zero
            heads = [zero] * (groups + 1)
            for b in reversed(range(groups)):
                heads[b] = head_const[b][part_of] + head_ratio[b] * heads[b + 1]
            for b in range(groups):
                below = last_const[b][part_of] + last_ratio[b] * heads[b]
                solved[b, part_of, 0] = below
                solved[b, part_of, 1] = heads[b + 1]
    below_re, above_re = solved[gz, 0, 0], solved[gz, 0, 1]
    below_im, above_im = solved[gz, 1, 0], solved[gz, 1, 1]

    def join(j, carry):
        rows_j = pl.ds(pl.multiple_of(j * RADIX, RADIX), RADIX)
        lo, hi = from_lo[rows_j, :], from_hi[rows_j, :]
        rhs_re[rows_j, :] = rhs_re[rows_j, :] + lo * below_re + hi * above_re
        rhs_im[rows_j, :] = rhs_im[rows_j, :] + lo * below_im + hi * above_im
        return carry

    scale = 1.0 / total_x
    sends_p = []
    own_p = []
    for z in range(depth // LANES):
        start = z * LANES
        cols = pl.ds(start, LANES)
        lax.fori_loop(start, start + LANES, join, 0, unroll=4)

        def inverse(k, carry):
            where = pl.ds(start * RADIX + k, LANES, stride=RADIX)
            line = jnp.concatenate([rhs_re[where, :], rhs_im[where, :]], axis=1)
            h, l = split(line)
            a, b = wh[k], wl[k]
            spec[k] = dot(a, h, over_last) + dot(b, h, over_last) + dot(a, l, over_last)
            return carry

        lax.fori_loop(0, RADIX, inverse, 0)

        def last_stage(t, carry):
            at = pl.multiple_of(t * 8, 8)
            re = [spec[k, pl.ds(at, 8), :] for k in range(RADIX)]
            im = [spec[k, pl.ds(inner + at, 8), :] for k in range(RADIX)]
            re, im = radix_eight(re, im, 1.0)
            for r in range(RADIX):
                back[0, pl.ds(r * inner + at, 8), cols] = re[r] * scale
                back[1, pl.ds(r * inner + at, 8), cols] = im[r] * scale
            return carry

        lax.fori_loop(0, inner // 8, last_stage, 0, unroll=2)
        for i in range(1, rows):
            theirs = pl.ds(pl.multiple_of(lax.rem(me + i, rows) * part, part), part)
            copy = to_row(
                back.at[:, theirs, cols], out.at[:, me, :, cols],
                p_send.at[z, i], p_recv.at[z, i], i,
            )
            copy.start()
            sends_p.append(copy)
        copy = pltpu.make_async_copy(
            back.at[:, mine, cols], out.at[:, me, :, cols], own_sem.at[2 + z]
        )
        copy.start()
        own_p.append(copy)
    for copy in own_p + sends_p:
        copy.wait()

    @pl.when(gz < groups - 1)
    def _():
        wall_copy.wait_send()


def on_device(rows, groups, velocity_x, velocity_y, velocity_z, spacing, level_index, plane_index):
    planes, part, depth = velocity_x.shape[1:]
    total_x = part * rows
    inner = total_x // RADIX
    assert planes == rows and depth % LANES == 0 and inner % LANES == 0
    high, low = phase_tables(total_x)
    bf16, f32 = jnp.bfloat16, jnp.float32
    vmem = pltpu.VMEM
    lines = (depth * RADIX, inner)
    dma = pltpu.SemaphoreType.DMA
    hbm = pl.BlockSpec(memory_space=pl.ANY)
    smem = pl.BlockSpec(memory_space=pltpu.SMEM)
    return pl.pallas_call(
        functools.partial(kernel, rows, groups),
        out_shape=jax.ShapeDtypeStruct(velocity_x.shape, f32),
        in_specs=[hbm] * 5 + [pl.BlockSpec(memory_space=pltpu.VMEM), smem, smem, smem],
        out_specs=hbm,
        scratch_shapes=[
            vmem(velocity_y.shape, bf16),
            vmem(velocity_z.shape, bf16),
            vmem(high.shape, bf16),
            vmem(high.shape, bf16),
            vmem((part, LANES), bf16),
            vmem((part, LANES), bf16),
            vmem((planes, 2, part, depth), bf16),
            vmem((2, total_x, depth), bf16),
            vmem((2, total_x, depth), bf16),
            vmem((RADIX, 2 * inner, depth), bf16),
            vmem((RADIX, 2 * inner, depth), bf16),
        ]
        + [vmem(lines, f32)] * 7
        + [
            vmem((groups, 4, RADIX, inner), f32),
            vmem((groups, 4, RADIX, inner), f32),
            vmem((groups, 2, 2, RADIX, inner), f32),
            vmem((RADIX, 2 * inner, LANES), f32),
            vmem((2, total_x, depth), f32),
            dma((4,)),
            dma((2 + depth // LANES,)),
            dma((rows,)), dma((rows,)), dma((rows,)), dma((rows,)),
            dma, dma,
            dma((groups,)), dma((groups,)), dma((groups,)), dma((groups,)),
            dma((depth // LANES, rows)), dma((depth // LANES, rows)),
        ],
        compiler_params=pltpu.CompilerParams(
            collective_id=0, has_side_effects=True, vmem_limit_bytes=56 * 1024 * 1024
        ),
    )(
        velocity_x, velocity_y, velocity_z, jnp.asarray(high), jnp.asarray(low),
        level_index.reshape(1, -1), spacing, level_index, plane_index,
    )


def solution(mesh):
    placed = (
        P(None, None, "row", "gz"),
        P(None, None, "row", "gz"),
        P(None, None, "row", "gz"),
        P(),
        P(),
        P(),
    )
    body = functools.partial(on_device, mesh.shape["row"], mesh.shape["gz"])
    return jax.shard_map(
        body, mesh=mesh, in_specs=placed, out_specs=P(None, None, "row", "gz"), check_vma=False
    )
```

```python
import functools
import math

import jax
import jax.numpy as jnp
import numpy as np
from jax import lax
from jax.experimental import pallas as pl
from jax.experimental.pallas import tpu as pltpu
from jax.sharding import PartitionSpec as P

RADIX = 8
LANES = 128

full_turn = 2.0 * math.pi
wave_unit = 2.0 * math.pi / 2048.0


def phase_tables(total_x):
    inner = total_x // RADIX
    k1 = np.arange(RADIX)[:, None, None]
    m = np.arange(inner)[None, :, None]
    k2 = np.arange(inner)[None, None, :]
    angle = -full_turn * ((m * (k1 + RADIX * k2)) % total_x) / total_x
    cos, sin = np.cos(angle), np.sin(angle)
    table = np.concatenate(
        [np.concatenate([cos, sin], axis=2), np.concatenate([-sin, cos], axis=2)], axis=1
    )
    high = table.astype(jnp.bfloat16)
    low = (table - high.astype(np.float64)).astype(jnp.bfloat16)
    return high, low


def radix_eight(re, im, sign):
    half = math.sqrt(0.5)
    add = lambda a, b: (a[0] + b[0], a[1] + b[1])
    sub = lambda a, b: (a[0] - b[0], a[1] - b[1])
    turn = lambda a: (-sign * a[1], sign * a[0])
    x = list(zip(re, im))
    even = [add(x[j], x[j + 4]) for j in range(4)]
    odd = [sub(x[j], x[j + 4]) for j in range(4)]
    a, b = odd[1]
    odd[1] = (half * (a - sign * b), half * (b + sign * a))
    odd[2] = turn(odd[2])
    a, b = odd[3]
    odd[3] = (half * (-a - sign * b), half * (sign * a - b))

    def four(v):
        t0, t1 = add(v[0], v[2]), sub(v[0], v[2])
        t2, t3 = add(v[1], v[3]), turn(sub(v[1], v[3]))
        return [add(t0, t2), add(t1, t3), sub(t0, t2), sub(t1, t3)]

    e, o = four(even), four(odd)
    out = [e[0], o[0], e[1], o[1], e[2], o[2], e[3], o[3]]
    return [v[0] for v in out], [v[1] for v in out]


def split(value):
    high = value.astype(jnp.bfloat16)
    return high, (value - high.astype(jnp.float32)).astype(jnp.bfloat16)


def kernel(
    rows, groups,
    vx, vy_hbm, vz_hbm, wh_hbm, wl_hbm, level_row, spacing, level, plane,
    out,
    vy, vz, wh, wl, wall_out, wall_in, src, got_u, got_s,
    yh, yl, rhs_re, rhs_im, qq, lq, uq, from_lo, from_hi, coef, edge, solved, spec, back,
    load_sem, own_sem, u_send, u_recv, s_send, s_recv, w_send, w_recv,
    c_send, c_recv, e_send, e_recv, p_send, p_recv,
):
    me = lax.axis_index("row")
    gz = lax.axis_index("gz")
    planes, part, depth = vx.shape[1:]
    total_x = part * rows
    inner = total_x // RADIX
    total_z = level.shape[0]
    levels = spacing.shape[0]
    f32 = jnp.float32

    loads = [
        pltpu.make_async_copy(vz_hbm, vz, load_sem.at[0]),
        pltpu.make_async_copy(vy_hbm, vy, load_sem.at[1]),
        pltpu.make_async_copy(wh_hbm, wh, load_sem.at[2]),
        pltpu.make_async_copy(wl_hbm, wl, load_sem.at[3]),
    ]
    for load in loads:
        load.start()
    mine = pl.ds(pl.multiple_of(me * part, part), part)
    own_u = pltpu.make_async_copy(vx.at[:, me], got_u.at[:, mine, :], own_sem.at[0])
    own_u.start()

    barrier = pltpu.get_barrier_semaphore()
    for i in range(1, rows):
        pl.semaphore_signal(
            barrier, inc=1, device_id={"row": lax.rem(me + i, rows)},
            device_id_type=pl.DeviceIdType.MESH,
        )
    for i in range(1, groups):
        pl.semaphore_signal(
            barrier, inc=1, device_id={"gz": lax.rem(gz + i, groups)},
            device_id_type=pl.DeviceIdType.MESH,
        )
    pl.semaphore_wait(barrier, rows + groups - 2)

    def to_row(source, target, send, recv, i):
        return pltpu.make_async_remote_copy(
            src_ref=source, dst_ref=target, send_sem=send, recv_sem=recv,
            device_id={"row": lax.rem(me + i, rows)}, device_id_type=pl.DeviceIdType.MESH,
        )

    def to_group(source, target, send, recv, i):
        return pltpu.make_async_remote_copy(
            src_ref=source, dst_ref=target, send_sem=send, recv_sem=recv,
            device_id={"gz": lax.rem(gz + i, groups)}, device_id_type=pl.DeviceIdType.MESH,
        )

    sends_u = []
    for i in range(1, rows):
        copy = to_row(
            vx.at[:, lax.rem(me + i, rows)], got_u.at[:, mine, :], u_send.at[i], u_recv.at[i], i
        )
        copy.start()
        sends_u.append(copy)

    lane_small = lax.broadcasted_iota(jnp.int32, (part, LANES), 1)
    loads[0].wait()
    packed = jnp.zeros((part, LANES), f32)
    for c in range(2):
        for p in range(planes):
            slot = c * planes + p
            tile = vz[c, p, :, depth - LANES :].astype(f32)
            packed = jnp.where(lane_small == slot, pltpu.roll(tile, (slot + 1) % LANES, 1), packed)
    wall_out[...] = packed.astype(jnp.bfloat16)
    wall_copy = to_group(wall_out, wall_in, w_send, w_recv, 1)

    @pl.when(gz < groups - 1)
    def _():
        wall_copy.start()

    base = gz * depth
    own_level = level_row[:, pl.ds(pl.multiple_of(base, LANES), depth)]
    width = jnp.zeros((1, depth), f32)
    for n in range(levels):
        width = jnp.where(own_level == n, spacing[n], width)
    loads[1].wait()

    @pl.when(gz > 0)
    def _():
        wall_copy.wait_recv()

    @pl.when(gz == 0)
    def _():
        wall_in[...] = jnp.zeros_like(wall_in)

    first_lane = lax.broadcasted_iota(jnp.int32, (part, depth), 1) == 0

    def slope_of(c, p):
        values = vz[c, p].astype(f32)
        slot = c * planes + p
        turned = pltpu.roll(wall_in[...].astype(f32), lax.rem(LANES - slot, LANES), 1)
        if depth > LANES:
            turned = jnp.concatenate([turned] * (depth // LANES), axis=1)
        below = jnp.where(first_lane, turned, pltpu.roll(values, 1, 1))
        return (values - below) / width

    def make_source(i, carry):
        p = lax.rem(me + i, rows)
        wave = jnp.full((1, depth), plane[p], jnp.int32).astype(f32) * wave_unit
        src[p, 0] = (-wave * vy[1, p].astype(f32) + slope_of(0, p)).astype(jnp.bfloat16)
        src[p, 1] = (wave * vy[0, p].astype(f32) + slope_of(1, p)).astype(jnp.bfloat16)

        @pl.when(i > 0)
        def _():
            to_row(src.at[p], got_s.at[:, mine, :], s_send.at[i], s_recv.at[i], i).start()

        return carry

    lax.fori_loop(1, rows, make_source, 0)
    make_source(0, 0)
    own_s = pltpu.make_async_copy(src.at[me], got_s.at[:, mine, :], own_sem.at[1])
    own_s.start()

    tile = (RADIX, inner)
    k1s = lax.broadcasted_iota(jnp.int32, tile, 0)
    k2s = lax.broadcasted_iota(jnp.int32, tile, 1)
    modes = k1s + RADIX * k2s
    wave_x = jnp.where(modes >= total_x // 2, modes - total_x, modes).astype(f32) * (
        full_turn / total_x
    )
    wave_y = jnp.full(tile, plane[me], jnp.int32).astype(f32) * wave_unit
    wave_sq = wave_x * wave_x + wave_y * wave_y

    def width_at(j):
        return jnp.full(tile, spacing[level[jnp.clip(j, 0, total_z - 1)]], f32)

    def factor(j, carry):
        excess, h_prev, h_now, homog = carry
        at = base + j
        h_next = width_at(at + 1)
        flag_lo = jnp.where(at > 0, 1.0, 0.0).astype(f32)
        flag_hi = jnp.where(at < total_z - 1, 1.0, 0.0).astype(f32)
        lower = flag_lo / (0.5 * (h_prev + h_now) * h_now)
        upper = flag_hi / (0.5 * (h_now + h_next) * h_now)
        s = wave_sq + lower * excess
        q = 1.0 / (upper + s)
        homog = lower * q * homog
        rows_j = pl.ds(pl.multiple_of(j * RADIX, RADIX), RADIX)
        qq[rows_j, :] = q
        lq[rows_j, :] = lower * q
        uq[rows_j, :] = upper * q
        from_lo[rows_j, :] = homog
        return s * q, h_now, h_next, homog

    one = jnp.ones(tile, f32)
    lax.fori_loop(0, depth, factor, (one, width_at(base - 1), width_at(base), one), unroll=4)

    def factor_back(t, carry):
        lo, hi = carry
        j = depth - 1 - t
        rows_j = pl.ds(pl.multiple_of(j * RADIX, RADIX), RADIX)
        ratio = uq[rows_j, :]
        lo = from_lo[rows_j, :] + ratio * lo
        hi = ratio * hi
        from_lo[rows_j, :] = lo
        from_hi[rows_j, :] = hi
        return lo, hi

    lax.fori_loop(0, depth, factor_back, (jnp.zeros(tile, f32), one), unroll=4)
    top = (depth - 1) * RADIX
    coef[gz, 0] = from_lo[0:RADIX, :]
    coef[gz, 1] = from_hi[0:RADIX, :]
    coef[gz, 2] = from_lo[top : top + RADIX, :]
    coef[gz, 3] = from_hi[top : top + RADIX, :]
    sends_c = []
    for i in range(1, groups):
        copy = to_group(coef.at[gz], coef.at[gz], c_send.at[i], c_recv.at[i], i)
        copy.start()
        sends_c.append(copy)

    step = 16

    def first_stage(field):
        def body(t, carry):
            at = pl.multiple_of(t * step, step)
            for lane in range(0, depth, LANES):
                cols = pl.ds(lane, LANES)
                re = [field[0, pl.ds(r * inner + at, step), cols].astype(f32) for r in range(RADIX)]
                im = [field[1, pl.ds(r * inner + at, step), cols].astype(f32) for r in range(RADIX)]
                re, im = radix_eight(re, im, -1.0)
                for k in range(RADIX):
                    h, l = split(re[k])
                    yh[k, pl.ds(at, step), cols] = h
                    yl[k, pl.ds(at, step), cols] = l
                    h, l = split(im[k])
                    yh[k, pl.ds(inner + at, step), cols] = h
                    yl[k, pl.ds(inner + at, step), cols] = l
            return carry

        lax.fori_loop(0, inner // step, body, 0)

    over_rows = (((0,), (0,)), ((), ()))
    over_last = (((1,), (1,)), ((), ()))

    def dot(a, b, dims):
        return lax.dot_general(a, b, dims, preferred_element_type=f32)

    def second_stage(combine):
        def body(k, carry):
            h, l, a, b = yh[k], yl[k], wh[k], wl[k]
            hat = dot(h, a, over_rows) + dot(h, b, over_rows) + dot(l, a, over_rows)
            combine(k, hat[:, :inner], hat[:, inner:])
            return carry

        lax.fori_loop(0, RADIX, body, 0)

    def put_along(k, re, im):
        number = k + RADIX * lax.broadcasted_iota(jnp.int32, (1, inner), 1)
        column = jnp.where(number >= total_x // 2, number - total_x, number).astype(f32) * (
            full_turn / total_x
        )
        where = pl.ds(k, depth, stride=RADIX)
        rhs_re[where, :] = -column * im
        rhs_im[where, :] = column * re

    def put_source(k, re, im):
        where = pl.ds(k, depth, stride=RADIX)
        rhs_re[where, :] = rhs_re[where, :] + re
        rhs_im[where, :] = rhs_im[where, :] + im

    own_u.wait()
    for copy in sends_u:
        copy.wait()
    for load in loads[2:]:
        load.wait()
    first_stage(got_u)
    second_stage(put_along)
    own_s.wait()
    for i in range(1, rows):
        to_row(
            src.at[lax.rem(me + i, rows)], got_s.at[:, mine, :], s_send.at[i], s_recv.at[i], i
        ).wait()
    first_stage(got_s)
    second_stage(put_source)

    def sweep(j, carry):
        re, im = carry
        rows_j = pl.ds(pl.multiple_of(j * RADIX, RADIX), RADIX)
        q, low = qq[rows_j, :], lq[rows_j, :]
        re = low * re - q * rhs_re[rows_j, :]
        im = low * im - q * rhs_im[rows_j, :]
        rhs_re[rows_j, :] = re
        rhs_im[rows_j, :] = im
        return re, im

    def sweep_back(t, carry):
        re, im = carry
        rows_j = pl.ds(pl.multiple_of((depth - 1 - t) * RADIX, RADIX), RADIX)
        ratio = uq[rows_j, :]
        re = rhs_re[rows_j, :] + ratio * re
        im = rhs_im[rows_j, :] + ratio * im
        rhs_re[rows_j, :] = re
        rhs_im[rows_j, :] = im
        return re, im

    zero = jnp.zeros(tile, f32)
    lax.fori_loop(0, depth, sweep, (zero, zero), unroll=4)
    lax.fori_loop(0, depth, sweep_back, (zero, zero), unroll=4)

    edge[gz, 0] = rhs_re[0:RADIX, :]
    edge[gz, 1] = rhs_re[top : top + RADIX, :]
    edge[gz, 2] = rhs_im[0:RADIX, :]
    edge[gz, 3] = rhs_im[top : top + RADIX, :]
    sends_e = []
    for i in range(1, groups):
        copy = to_group(edge.at[gz], edge.at[gz], e_send.at[i], e_recv.at[i], i)
        copy.start()
        sends_e.append(copy)
    for copy in sends_c:
        copy.wait()
    for copy in sends_e:
        copy.wait()
    if True:
        last_const, last_ratio = [(zero, zero)], [zero]
        head_const, head_ratio = [], []
        for b in range(groups):
            a0, b0, a1, b1 = (coef[b, n] for n in range(4))
            inv = 1.0 / (1.0 - a0 * last_ratio[b])
            ratio = b0 * inv
            head_ratio.append(ratio)
            heads, lasts = [], []
            for part_of in range(2):
                prev = last_const[b][part_of]
                head = (edge[b, 2 * part_of] + a0 * prev) * inv
                heads.append(head)
                lasts.append(edge[b, 2 * part_of + 1] + a1 * (prev + last_ratio[b] * head))
            head_const.append(heads)
            last_const.append(lasts)
            last_ratio.append(a1 * last_ratio[b] * ratio + b1)
        for part_of in range(2):
            following = zero
            heads = [zero] * (groups + 1)
            for b in reversed(range(groups)):
                heads[b] = head_const[b][part_of] + head_ratio[b] * heads[b + 1]
            for b in range(groups):
                below = last_const[b][part_of] + last_ratio[b] * heads[b]
                solved[b, part_of, 0] = below
                solved[b, part_of, 1] = heads[b + 1]
    below_re, above_re = solved[gz, 0, 0], solved[gz, 0, 1]
    below_im, above_im = solved[gz, 1, 0], solved[gz, 1, 1]

    def join(j, carry):
        rows_j = pl.ds(pl.multiple_of(j * RADIX, RADIX), RADIX)
        lo, hi = from_lo[rows_j, :], from_hi[rows_j, :]
        rhs_re[rows_j, :] = rhs_re[rows_j, :] + lo * below_re + hi * above_re
        rhs_im[rows_j, :] = rhs_im[rows_j, :] + lo * below_im + hi * above_im
        return carry

    scale = 1.0 / total_x
    sends_p = []
    own_p = []
    for z in range(depth // LANES):
        start = z * LANES
        cols = pl.ds(start, LANES)
        lax.fori_loop(start, start + LANES, join, 0, unroll=4)

        def inverse(k, carry):
            where = pl.ds(start * RADIX + k, LANES, stride=RADIX)
            line = jnp.concatenate([rhs_re[where, :], rhs_im[where, :]], axis=1)
            h, l = split(line)
            a, b = wh[k], wl[k]
            spec[k] = dot(a, h, over_last) + dot(b, h, over_last) + dot(a, l, over_last)
            return carry

        lax.fori_loop(0, RADIX, inverse, 0)

        def last_stage(t, carry):
            at = pl.multiple_of(t * step, step)
            re = [spec[k, pl.ds(at, step), :] for k in range(RADIX)]
            im = [spec[k, pl.ds(inner + at, step), :] for k in range(RADIX)]
            re, im = radix_eight(re, im, 1.0)
            for r in range(RADIX):
                back[0, pl.ds(r * inner + at, step), cols] = (re[r] * scale).astype(jnp.bfloat16)
                back[1, pl.ds(r * inner + at, step), cols] = (im[r] * scale).astype(jnp.bfloat16)
            return carry

        lax.fori_loop(0, inner // step, last_stage, 0)
        for i in range(1, rows):
            theirs = pl.ds(pl.multiple_of(lax.rem(me + i, rows) * part, part), part)
            copy = to_row(
                back.at[:, theirs, cols], out.at[:, me, :, cols],
                p_send.at[z, i], p_recv.at[z, i], i,
            )
            copy.start()
            sends_p.append(copy)
        copy = pltpu.make_async_copy(
            back.at[:, mine, cols], out.at[:, me, :, cols], own_sem.at[2 + z]
        )
        copy.start()
        own_p.append(copy)
    for copy in own_p + sends_p:
        copy.wait()

    @pl.when(gz < groups - 1)
    def _():
        wall_copy.wait_send()


def on_device(rows, groups, velocity_x, velocity_y, velocity_z, spacing, level_index, plane_index):
    planes, part, depth = velocity_x.shape[1:]
    total_x = part * rows
    inner = total_x // RADIX
    assert planes == rows and depth % LANES == 0 and inner % LANES == 0
    high, low = phase_tables(total_x)
    bf16, f32 = jnp.bfloat16, jnp.float32
    vmem = pltpu.VMEM
    lines = (depth * RADIX, inner)
    dma = pltpu.SemaphoreType.DMA
    hbm = pl.BlockSpec(memory_space=pl.ANY)
    smem = pl.BlockSpec(memory_space=pltpu.SMEM)
    received = pl.pallas_call(
        functools.partial(kernel, rows, groups),
        out_shape=jax.ShapeDtypeStruct(velocity_x.shape, bf16),
        in_specs=[hbm] * 5 + [pl.BlockSpec(memory_space=pltpu.VMEM), smem, smem, smem],
        out_specs=hbm,
        scratch_shapes=[
            vmem(velocity_y.shape, bf16),
            vmem(velocity_z.shape, bf16),
            vmem(high.shape, bf16),
            vmem(high.shape, bf16),
            vmem((part, LANES), bf16),
            vmem((part, LANES), bf16),
            vmem((planes, 2, part, depth), bf16),
            vmem((2, total_x, depth), bf16),
            vmem((2, total_x, depth), bf16),
            vmem((RADIX, 2 * inner, depth), bf16),
            vmem((RADIX, 2 * inner, depth), bf16),
        ]
        + [vmem(lines, f32)] * 7
        + [
            vmem((groups, 4, RADIX, inner), f32),
            vmem((groups, 4, RADIX, inner), f32),
            vmem((groups, 2, 2, RADIX, inner), f32),
            vmem((RADIX, 2 * inner, LANES), f32),
            vmem((2, total_x, depth), bf16),
            dma((4,)),
            dma((2 + depth // LANES,)),
            dma((rows,)), dma((rows,)), dma((rows,)), dma((rows,)),
            dma, dma,
            dma((groups,)), dma((groups,)), dma((groups,)), dma((groups,)),
            dma((depth // LANES, rows)), dma((depth // LANES, rows)),
        ],
        compiler_params=pltpu.CompilerParams(
            collective_id=0, has_side_effects=True, vmem_limit_bytes=56 * 1024 * 1024
        ),
    )(
        velocity_x, velocity_y, velocity_z, jnp.asarray(high), jnp.asarray(low),
        level_index.reshape(1, -1), spacing, level_index, plane_index,
    )
    return received.astype(f32)


def solution(mesh):
    placed = (
        P(None, None, "row", "gz"),
        P(None, None, "row", "gz"),
        P(None, None, "row", "gz"),
        P(),
        P(),
        P(),
    )
    body = functools.partial(on_device, mesh.shape["row"], mesh.shape["gz"])
    return jax.shard_map(
        body, mesh=mesh, in_specs=placed, out_specs=P(None, None, "row", "gz"), check_vma=False
    )
```

```python
import functools
import math

import jax
import jax.numpy as jnp
import numpy as np
from jax import lax
from jax.experimental import pallas as pl
from jax.experimental.pallas import tpu as pltpu
from jax.sharding import PartitionSpec as P

RADIX = 8
LANES = 128

full_turn = 2.0 * math.pi
wave_unit = 2.0 * math.pi / 2048.0


def phase_tables(total_x):
    inner = total_x // RADIX
    k1 = np.arange(RADIX)[:, None, None]
    m = np.arange(inner)[None, :, None]
    k2 = np.arange(inner)[None, None, :]
    angle = -full_turn * ((m * (k1 + RADIX * k2)) % total_x) / total_x
    cos, sin = np.cos(angle), np.sin(angle)
    table = np.concatenate(
        [np.concatenate([cos, sin], axis=2), np.concatenate([-sin, cos], axis=2)], axis=1
    )
    high = table.astype(jnp.bfloat16)
    low = (table - high.astype(np.float64)).astype(jnp.bfloat16)
    return high, low


def radix_eight(re, im, sign):
    half = math.sqrt(0.5)
    add = lambda a, b: (a[0] + b[0], a[1] + b[1])
    sub = lambda a, b: (a[0] - b[0], a[1] - b[1])
    turn = lambda a: (-sign * a[1], sign * a[0])
    x = list(zip(re, im))
    even = [add(x[j], x[j + 4]) for j in range(4)]
    odd = [sub(x[j], x[j + 4]) for j in range(4)]
    a, b = odd[1]
    odd[1] = (half * (a - sign * b), half * (b + sign * a))
    odd[2] = turn(odd[2])
    a, b = odd[3]
    odd[3] = (half * (-a - sign * b), half * (sign * a - b))

    def four(v):
        t0, t1 = add(v[0], v[2]), sub(v[0], v[2])
        t2, t3 = add(v[1], v[3]), turn(sub(v[1], v[3]))
        return [add(t0, t2), add(t1, t3), sub(t0, t2), sub(t1, t3)]

    e, o = four(even), four(odd)
    out = [e[0], o[0], e[1], o[1], e[2], o[2], e[3], o[3]]
    return [v[0] for v in out], [v[1] for v in out]


def split(value):
    high = value.astype(jnp.bfloat16)
    return high, (value - high.astype(jnp.float32)).astype(jnp.bfloat16)


def kernel(
    rows, groups,
    vx, vy_hbm, vz_hbm, wh_hbm, wl_hbm, level_row, spacing, level, plane,
    out,
    vy, vz, wh, wl, wall_out, wall_in, src, got_u, got_s,
    yh, yl, rhs_re, rhs_im, qq, lq, uq, from_lo, from_hi, coef, edge, solved, spec, back,
    load_sem, own_sem, u_send, u_recv, s_send, s_recv, w_send, w_recv,
    c_send, c_recv, e_send, e_recv, p_send, p_recv,
):
    me = lax.axis_index("row")
    gz = lax.axis_index("gz")
    planes, part, depth = vx.shape[1:]
    total_x = part * rows
    inner = total_x // RADIX
    total_z = level.shape[0]
    levels = spacing.shape[0]
    f32 = jnp.float32

    loads = [
        pltpu.make_async_copy(vz_hbm, vz, load_sem.at[0]),
        pltpu.make_async_copy(vy_hbm, vy, load_sem.at[1]),
        pltpu.make_async_copy(wh_hbm, wh, load_sem.at[2]),
        pltpu.make_async_copy(wl_hbm, wl, load_sem.at[3]),
    ]
    for load in loads:
        load.start()
    mine = pl.ds(pl.multiple_of(me * part, part), part)
    own_u = pltpu.make_async_copy(vx.at[:, me], got_u.at[:, mine, :], own_sem.at[0])
    own_u.start()

    barrier = pltpu.get_barrier_semaphore()
    for i in range(1, rows):
        pl.semaphore_signal(
            barrier, inc=1, device_id={"row": lax.rem(me + i, rows)},
            device_id_type=pl.DeviceIdType.MESH,
        )
    for i in range(1, groups):
        pl.semaphore_signal(
            barrier, inc=1, device_id={"gz": lax.rem(gz + i, groups)},
            device_id_type=pl.DeviceIdType.MESH,
        )
    pl.semaphore_wait(barrier, rows + groups - 2)

    def to_row(source, target, send, recv, i):
        return pltpu.make_async_remote_copy(
            src_ref=source, dst_ref=target, send_sem=send, recv_sem=recv,
            device_id={"row": lax.rem(me + i, rows)}, device_id_type=pl.DeviceIdType.MESH,
        )

    def to_group(source, target, send, recv, i):
        return pltpu.make_async_remote_copy(
            src_ref=source, dst_ref=target, send_sem=send, recv_sem=recv,
            device_id={"gz": lax.rem(gz + i, groups)}, device_id_type=pl.DeviceIdType.MESH,
        )

    sends_u = []
    for i in range(1, rows):
        copy = to_row(
            vx.at[:, lax.rem(me + i, rows)], got_u.at[:, mine, :], u_send.at[i], u_recv.at[i], i
        )
        copy.start()
        sends_u.append(copy)

    lane_small = lax.broadcasted_iota(jnp.int32, (part, LANES), 1)
    loads[0].wait()
    packed = jnp.zeros((part, LANES), f32)
    for c in range(2):
        for p in range(planes):
            slot = c * planes + p
            tile = vz[c, p, :, depth - LANES :].astype(f32)
            packed = jnp.where(lane_small == slot, pltpu.roll(tile, (slot + 1) % LANES, 1), packed)
    wall_out[...] = packed.astype(jnp.bfloat16)
    wall_copy = to_group(wall_out, wall_in, w_send, w_recv, 1)

    @pl.when(gz < groups - 1)
    def _():
        wall_copy.start()

    base = gz * depth
    own_level = level_row[:, pl.ds(pl.multiple_of(base, LANES), depth)]
    width = jnp.zeros((1, depth), f32)
    for n in range(levels):
        width = jnp.where(own_level == n, spacing[n], width)
    loads[1].wait()

    @pl.when(gz > 0)
    def _():
        wall_copy.wait_recv()

    @pl.when(gz == 0)
    def _():
        wall_in[...] = jnp.zeros_like(wall_in)

    first_lane = lax.broadcasted_iota(jnp.int32, (part, depth), 1) == 0

    def slope_of(c, p):
        values = vz[c, p].astype(f32)
        slot = c * planes + p
        turned = pltpu.roll(wall_in[...].astype(f32), lax.rem(LANES - slot, LANES), 1)
        if depth > LANES:
            turned = jnp.concatenate([turned] * (depth // LANES), axis=1)
        below = jnp.where(first_lane, turned, pltpu.roll(values, 1, 1))
        return (values - below) / width

    def make_source(i, carry):
        p = lax.rem(me + i, rows)
        wave = jnp.full((1, depth), plane[p], jnp.int32).astype(f32) * wave_unit
        src[p, 0] = (-wave * vy[1, p].astype(f32) + slope_of(0, p)).astype(jnp.bfloat16)
        src[p, 1] = (wave * vy[0, p].astype(f32) + slope_of(1, p)).astype(jnp.bfloat16)

        @pl.when(i > 0)
        def _():
            to_row(src.at[p], got_s.at[:, mine, :], s_send.at[i], s_recv.at[i], i).start()

        return carry

    lax.fori_loop(1, rows, make_source, 0)
    make_source(0, 0)
    own_s = pltpu.make_async_copy(src.at[me], got_s.at[:, mine, :], own_sem.at[1])
    own_s.start()

    tile = (RADIX, inner)
    k1s = lax.broadcasted_iota(jnp.int32, tile, 0)
    k2s = lax.broadcasted_iota(jnp.int32, tile, 1)
    modes = k1s + RADIX * k2s
    wave_x = jnp.where(modes >= total_x // 2, modes - total_x, modes).astype(f32) * (
        full_turn / total_x
    )
    wave_y = jnp.full(tile, plane[me], jnp.int32).astype(f32) * wave_unit
    wave_sq = wave_x * wave_x + wave_y * wave_y

    def width_at(j):
        return jnp.full(tile, spacing[level[jnp.clip(j, 0, total_z - 1)]], f32)

    def factor(j, carry):
        excess, h_prev, h_now, homog = carry
        at = base + j
        h_next = width_at(at + 1)
        flag_lo = jnp.where(at > 0, 1.0, 0.0).astype(f32)
        flag_hi = jnp.where(at < total_z - 1, 1.0, 0.0).astype(f32)
        lower = flag_lo / (0.5 * (h_prev + h_now) * h_now)
        upper = flag_hi / (0.5 * (h_now + h_next) * h_now)
        s = wave_sq + lower * excess
        q = 1.0 / (upper + s)
        homog = lower * q * homog
        rows_j = pl.ds(pl.multiple_of(j * RADIX, RADIX), RADIX)
        qq[rows_j, :] = q
        lq[rows_j, :] = lower * q
        uq[rows_j, :] = upper * q
        from_lo[rows_j, :] = homog
        return s * q, h_now, h_next, homog

    one = jnp.ones(tile, f32)
    lax.fori_loop(0, depth, factor, (one, width_at(base - 1), width_at(base), one), unroll=8)

    def factor_back(t, carry):
        lo, hi = carry
        j = depth - 1 - t
        rows_j = pl.ds(pl.multiple_of(j * RADIX, RADIX), RADIX)
        ratio = uq[rows_j, :]
        lo = from_lo[rows_j, :] + ratio * lo
        hi = ratio * hi
        from_lo[rows_j, :] = lo
        from_hi[rows_j, :] = hi
        return lo, hi

    lax.fori_loop(0, depth, factor_back, (jnp.zeros(tile, f32), one), unroll=16)
    top = (depth - 1) * RADIX
    coef[gz, 0] = from_lo[0:RADIX, :]
    coef[gz, 1] = from_hi[0:RADIX, :]
    coef[gz, 2] = from_lo[top : top + RADIX, :]
    coef[gz, 3] = from_hi[top : top + RADIX, :]
    sends_c = []
    for i in range(1, groups):
        copy = to_group(coef.at[gz], coef.at[gz], c_send.at[i], c_recv.at[i], i)
        copy.start()
        sends_c.append(copy)

    step = 16

    def first_stage(field):
        def body(t, carry):
            at = pl.multiple_of(t * step, step)
            for lane in range(0, depth, LANES):
                cols = pl.ds(lane, LANES)
                re = [field[0, pl.ds(r * inner + at, step), cols].astype(f32) for r in range(RADIX)]
                im = [field[1, pl.ds(r * inner + at, step), cols].astype(f32) for r in range(RADIX)]
                re, im = radix_eight(re, im, -1.0)
                for k in range(RADIX):
                    h, l = split(re[k])
                    yh[k, pl.ds(at, step), cols] = h
                    yl[k, pl.ds(at, step), cols] = l
                    h, l = split(im[k])
                    yh[k, pl.ds(inner + at, step), cols] = h
                    yl[k, pl.ds(inner + at, step), cols] = l
            return carry

        lax.fori_loop(0, inner // step, body, 0)

    over_rows = (((0,), (0,)), ((), ()))
    over_last = (((1,), (1,)), ((), ()))

    def dot(a, b, dims):
        return lax.dot_general(a, b, dims, preferred_element_type=f32)

    def second_stage(combine):
        def body(k, carry):
            h, l, a, b = yh[k], yl[k], wh[k], wl[k]
            hat = dot(h, a, over_rows) + dot(h, b, over_rows) + dot(l, a, over_rows)
            combine(k, hat[:, :inner], hat[:, inner:])
            return carry

        lax.fori_loop(0, RADIX, body, 0, unroll=4)

    def put_along(k, re, im):
        number = k + RADIX * lax.broadcasted_iota(jnp.int32, (1, inner), 1)
        column = jnp.where(number >= total_x // 2, number - total_x, number).astype(f32) * (
            full_turn / total_x
        )
        where = pl.ds(k, depth, stride=RADIX)
        rhs_re[where, :] = -column * im
        rhs_im[where, :] = column * re

    def put_source(k, re, im):
        where = pl.ds(k, depth, stride=RADIX)
        rhs_re[where, :] = rhs_re[where, :] + re
        rhs_im[where, :] = rhs_im[where, :] + im

    own_u.wait()
    for copy in sends_u:
        copy.wait()
    for load in loads[2:]:
        load.wait()
    first_stage(got_u)
    second_stage(put_along)
    own_s.wait()
    for i in range(1, rows):
        to_row(
            src.at[lax.rem(me + i, rows)], got_s.at[:, mine, :], s_send.at[i], s_recv.at[i], i
        ).wait()
    first_stage(got_s)
    second_stage(put_source)

    def sweep(j, carry):
        re, im = carry
        rows_j = pl.ds(pl.multiple_of(j * RADIX, RADIX), RADIX)
        q, low = qq[rows_j, :], lq[rows_j, :]
        re = low * re - q * rhs_re[rows_j, :]
        im = low * im - q * rhs_im[rows_j, :]
        rhs_re[rows_j, :] = re
        rhs_im[rows_j, :] = im
        return re, im

    def sweep_back(t, carry):
        re, im = carry
        rows_j = pl.ds(pl.multiple_of((depth - 1 - t) * RADIX, RADIX), RADIX)
        ratio = uq[rows_j, :]
        re = rhs_re[rows_j, :] + ratio * re
        im = rhs_im[rows_j, :] + ratio * im
        rhs_re[rows_j, :] = re
        rhs_im[rows_j, :] = im
        return re, im

    zero = jnp.zeros(tile, f32)
    lax.fori_loop(0, depth, sweep, (zero, zero), unroll=16)
    lax.fori_loop(0, depth, sweep_back, (zero, zero), unroll=16)

    edge[gz, 0] = rhs_re[0:RADIX, :]
    edge[gz, 1] = rhs_re[top : top + RADIX, :]
    edge[gz, 2] = rhs_im[0:RADIX, :]
    edge[gz, 3] = rhs_im[top : top + RADIX, :]
    sends_e = []
    for i in range(1, groups):
        copy = to_group(edge.at[gz], edge.at[gz], e_send.at[i], e_recv.at[i], i)
        copy.start()
        sends_e.append(copy)
    for copy in sends_c:
        copy.wait()
    for copy in sends_e:
        copy.wait()
    if True:
        last_const, last_ratio = [(zero, zero)], [zero]
        head_const, head_ratio = [], []
        for b in range(groups):
            a0, b0, a1, b1 = (coef[b, n] for n in range(4))
            inv = 1.0 / (1.0 - a0 * last_ratio[b])
            ratio = b0 * inv
            head_ratio.append(ratio)
            heads, lasts = [], []
            for part_of in range(2):
                prev = last_const[b][part_of]
                head = (edge[b, 2 * part_of] + a0 * prev) * inv
                heads.append(head)
                lasts.append(edge[b, 2 * part_of + 1] + a1 * (prev + last_ratio[b] * head))
            head_const.append(heads)
            last_const.append(lasts)
            last_ratio.append(a1 * last_ratio[b] * ratio + b1)
        for part_of in range(2):
            following = zero
            heads = [zero] * (groups + 1)
            for b in reversed(range(groups)):
                heads[b] = head_const[b][part_of] + head_ratio[b] * heads[b + 1]
            for b in range(groups):
                below = last_const[b][part_of] + last_ratio[b] * heads[b]
                solved[b, part_of, 0] = below
                solved[b, part_of, 1] = heads[b + 1]
    below_re, above_re = solved[gz, 0, 0], solved[gz, 0, 1]
    below_im, above_im = solved[gz, 1, 0], solved[gz, 1, 1]

    def join(j, carry):
        rows_j = pl.ds(pl.multiple_of(j * RADIX, RADIX), RADIX)
        lo, hi = from_lo[rows_j, :], from_hi[rows_j, :]
        rhs_re[rows_j, :] = rhs_re[rows_j, :] + lo * below_re + hi * above_re
        rhs_im[rows_j, :] = rhs_im[rows_j, :] + lo * below_im + hi * above_im
        return carry

    scale = 1.0 / total_x
    sends_p = []
    own_p = []
    for z in range(depth // LANES):
        start = z * LANES
        cols = pl.ds(start, LANES)
        lax.fori_loop(start, start + LANES, join, 0, unroll=16)

        def inverse(k, carry):
            where = pl.ds(start * RADIX + k, LANES, stride=RADIX)
            line = jnp.concatenate([rhs_re[where, :], rhs_im[where, :]], axis=1)
            h, l = split(line)
            a, b = wh[k], wl[k]
            spec[k] = dot(a, h, over_last) + dot(b, h, over_last) + dot(a, l, over_last)
            return carry

        lax.fori_loop(0, RADIX, inverse, 0, unroll=4)

        def last_stage(t, carry):
            at = pl.multiple_of(t * step, step)
            re = [spec[k, pl.ds(at, step), :] for k in range(RADIX)]
            im = [spec[k, pl.ds(inner + at, step), :] for k in range(RADIX)]
            re, im = radix_eight(re, im, 1.0)
            for r in range(RADIX):
                back[0, pl.ds(r * inner + at, step), cols] = (re[r] * scale).astype(jnp.bfloat16)
                back[1, pl.ds(r * inner + at, step), cols] = (im[r] * scale).astype(jnp.bfloat16)
            return carry

        lax.fori_loop(0, inner // step, last_stage, 0)
        for i in range(1, rows):
            theirs = pl.ds(pl.multiple_of(lax.rem(me + i, rows) * part, part), part)
            copy = to_row(
                back.at[:, theirs, cols], out.at[:, me, :, cols],
                p_send.at[z, i], p_recv.at[z, i], i,
            )
            copy.start()
            sends_p.append(copy)
        copy = pltpu.make_async_copy(
            back.at[:, mine, cols], out.at[:, me, :, cols], own_sem.at[2 + z]
        )
        copy.start()
        own_p.append(copy)
    for copy in own_p + sends_p:
        copy.wait()

    @pl.when(gz < groups - 1)
    def _():
        wall_copy.wait_send()


def on_device(rows, groups, velocity_x, velocity_y, velocity_z, spacing, level_index, plane_index):
    planes, part, depth = velocity_x.shape[1:]
    total_x = part * rows
    inner = total_x // RADIX
    assert planes == rows and depth % LANES == 0 and inner % LANES == 0
    high, low = phase_tables(total_x)
    bf16, f32 = jnp.bfloat16, jnp.float32
    vmem = pltpu.VMEM
    lines = (depth * RADIX, inner)
    dma = pltpu.SemaphoreType.DMA
    hbm = pl.BlockSpec(memory_space=pl.ANY)
    smem = pl.BlockSpec(memory_space=pltpu.SMEM)
    received = pl.pallas_call(
        functools.partial(kernel, rows, groups),
        out_shape=jax.ShapeDtypeStruct(velocity_x.shape, bf16),
        in_specs=[hbm] * 5 + [pl.BlockSpec(memory_space=pltpu.VMEM), smem, smem, smem],
        out_specs=hbm,
        scratch_shapes=[
            vmem(velocity_y.shape, bf16),
            vmem(velocity_z.shape, bf16),
            vmem(high.shape, bf16),
            vmem(high.shape, bf16),
            vmem((part, LANES), bf16),
            vmem((part, LANES), bf16),
            vmem((planes, 2, part, depth), bf16),
            vmem((2, total_x, depth), bf16),
            vmem((2, total_x, depth), bf16),
            vmem((RADIX, 2 * inner, depth), bf16),
            vmem((RADIX, 2 * inner, depth), bf16),
        ]
        + [vmem(lines, f32)] * 7
        + [
            vmem((groups, 4, RADIX, inner), f32),
            vmem((groups, 4, RADIX, inner), f32),
            vmem((groups, 2, 2, RADIX, inner), f32),
            vmem((RADIX, 2 * inner, LANES), f32),
            vmem((2, total_x, depth), bf16),
            dma((4,)),
            dma((2 + depth // LANES,)),
            dma((rows,)), dma((rows,)), dma((rows,)), dma((rows,)),
            dma, dma,
            dma((groups,)), dma((groups,)), dma((groups,)), dma((groups,)),
            dma((depth // LANES, rows)), dma((depth // LANES, rows)),
        ],
        compiler_params=pltpu.CompilerParams(
            collective_id=0, has_side_effects=True, vmem_limit_bytes=56 * 1024 * 1024
        ),
    )(
        velocity_x, velocity_y, velocity_z, jnp.asarray(high), jnp.asarray(low),
        level_index.reshape(1, -1), spacing, level_index, plane_index,
    )
    return received.astype(f32)


def solution(mesh):
    placed = (
        P(None, None, "row", "gz"),
        P(None, None, "row", "gz"),
        P(None, None, "row", "gz"),
        P(),
        P(),
        P(),
    )
    body = functools.partial(on_device, mesh.shape["row"], mesh.shape["gz"])
    return jax.shard_map(
        body, mesh=mesh, in_specs=placed, out_specs=P(None, None, "row", "gz"), check_vma=False
    )
```

```python
import functools
import math

import jax
import jax.numpy as jnp
import numpy as np
from jax import lax
from jax.experimental import pallas as pl
from jax.experimental.pallas import tpu as pltpu
from jax.sharding import PartitionSpec as P

RADIX = 8
LANES = 128

full_turn = 2.0 * math.pi
wave_unit = 2.0 * math.pi / 2048.0


def phase_tables(total_x):
    inner = total_x // RADIX
    k1 = np.arange(RADIX)[:, None, None]
    m = np.arange(inner)[None, :, None]
    k2 = np.arange(inner)[None, None, :]
    angle = -full_turn * ((m * (k1 + RADIX * k2)) % total_x) / total_x
    cos, sin = np.cos(angle), np.sin(angle)
    table = np.concatenate(
        [np.concatenate([cos, sin], axis=2), np.concatenate([-sin, cos], axis=2)], axis=1
    )
    high = table.astype(jnp.bfloat16)
    low = (table - high.astype(np.float64)).astype(jnp.bfloat16)
    return high, low


def radix_eight(re, im, sign):
    half = math.sqrt(0.5)
    add = lambda a, b: (a[0] + b[0], a[1] + b[1])
    sub = lambda a, b: (a[0] - b[0], a[1] - b[1])
    turn = lambda a: (-sign * a[1], sign * a[0])
    x = list(zip(re, im))
    even = [add(x[j], x[j + 4]) for j in range(4)]
    odd = [sub(x[j], x[j + 4]) for j in range(4)]
    a, b = odd[1]
    odd[1] = (half * (a - sign * b), half * (b + sign * a))
    odd[2] = turn(odd[2])
    a, b = odd[3]
    odd[3] = (half * (-a - sign * b), half * (sign * a - b))

    def four(v):
        t0, t1 = add(v[0], v[2]), sub(v[0], v[2])
        t2, t3 = add(v[1], v[3]), turn(sub(v[1], v[3]))
        return [add(t0, t2), add(t1, t3), sub(t0, t2), sub(t1, t3)]

    e, o = four(even), four(odd)
    out = [e[0], o[0], e[1], o[1], e[2], o[2], e[3], o[3]]
    return [v[0] for v in out], [v[1] for v in out]


def split(value):
    high = value.astype(jnp.bfloat16)
    return high, (value - high.astype(jnp.float32)).astype(jnp.bfloat16)


def kernel(
    rows, groups,
    vx, vy_hbm, vz_hbm, wh_hbm, wl_hbm, level_row, spacing, level, plane,
    out,
    vy, vz, wh, wl, wall_out, wall_in, src, got_u, got_s,
    yh, yl, rhs_re, rhs_im, qq, lq, uq, from_lo, from_hi, coef, edge, solved, spec, back,
    load_sem, own_sem, u_send, u_recv, s_send, s_recv, w_send, w_recv,
    c_send, c_recv, e_send, e_recv, p_send, p_recv,
):
    me = lax.axis_index("row")
    gz = lax.axis_index("gz")
    planes, part, depth = vx.shape[1:]
    total_x = part * rows
    inner = total_x // RADIX
    total_z = level.shape[0]
    levels = spacing.shape[0]
    f32 = jnp.float32

    loads = [
        pltpu.make_async_copy(vz_hbm, vz, load_sem.at[0]),
        pltpu.make_async_copy(vy_hbm, vy, load_sem.at[1]),
        pltpu.make_async_copy(wh_hbm, wh, load_sem.at[2]),
        pltpu.make_async_copy(wl_hbm, wl, load_sem.at[3]),
    ]
    for load in loads:
        load.start()
    mine = pl.ds(pl.multiple_of(me * part, part), part)
    own_u = pltpu.make_async_copy(vx.at[:, me], got_u.at[:, mine, :], own_sem.at[0])
    own_u.start()

    barrier = pltpu.get_barrier_semaphore()
    for i in range(1, rows):
        pl.semaphore_signal(
            barrier, inc=1, device_id={"row": lax.rem(me + i, rows)},
            device_id_type=pl.DeviceIdType.MESH,
        )
    for i in range(1, groups):
        pl.semaphore_signal(
            barrier, inc=1, device_id={"gz": lax.rem(gz + i, groups)},
            device_id_type=pl.DeviceIdType.MESH,
        )
    pl.semaphore_wait(barrier, rows + groups - 2)

    def to_row(source, target, send, recv, i):
        return pltpu.make_async_remote_copy(
            src_ref=source, dst_ref=target, send_sem=send, recv_sem=recv,
            device_id={"row": lax.rem(me + i, rows)}, device_id_type=pl.DeviceIdType.MESH,
        )

    def to_group(source, target, send, recv, i):
        return pltpu.make_async_remote_copy(
            src_ref=source, dst_ref=target, send_sem=send, recv_sem=recv,
            device_id={"gz": lax.rem(gz + i, groups)}, device_id_type=pl.DeviceIdType.MESH,
        )

    sends_u = []
    for i in range(1, rows):
        copy = to_row(
            vx.at[:, lax.rem(me + i, rows)], got_u.at[:, mine, :], u_send.at[i], u_recv.at[i], i
        )
        copy.start()
        sends_u.append(copy)

    lane_small = lax.broadcasted_iota(jnp.int32, (part, LANES), 1)
    loads[0].wait()
    packed = jnp.zeros((part, LANES), f32)
    for c in range(2):
        for p in range(planes):
            slot = c * planes + p
            tile = vz[c, p, :, depth - LANES :].astype(f32)
            packed = jnp.where(lane_small == slot, pltpu.roll(tile, (slot + 1) % LANES, 1), packed)
    wall_out[...] = packed.astype(jnp.bfloat16)
    wall_copy = to_group(wall_out, wall_in, w_send, w_recv, 1)

    @pl.when(gz < groups - 1)
    def _():
        wall_copy.start()

    base = gz * depth
    own_level = level_row[:, pl.ds(pl.multiple_of(base, LANES), depth)]
    width = jnp.zeros((1, depth), f32)
    for n in range(levels):
        width = jnp.where(own_level == n, spacing[n], width)
    loads[1].wait()

    @pl.when(gz > 0)
    def _():
        wall_copy.wait_recv()

    @pl.when(gz == 0)
    def _():
        wall_in[...] = jnp.zeros_like(wall_in)

    first_lane = lax.broadcasted_iota(jnp.int32, (part, depth), 1) == 0

    def slope_of(c, p):
        values = vz[c, p].astype(f32)
        slot = c * planes + p
        turned = pltpu.roll(wall_in[...].astype(f32), lax.rem(LANES - slot, LANES), 1)
        if depth > LANES:
            turned = jnp.concatenate([turned] * (depth // LANES), axis=1)
        below = jnp.where(first_lane, turned, pltpu.roll(values, 1, 1))
        return (values - below) / width

    def make_source(i, carry):
        p = lax.rem(me + i, rows)
        wave = jnp.full((1, depth), plane[p], jnp.int32).astype(f32) * wave_unit
        src[p, 0] = (-wave * vy[1, p].astype(f32) + slope_of(0, p)).astype(jnp.bfloat16)
        src[p, 1] = (wave * vy[0, p].astype(f32) + slope_of(1, p)).astype(jnp.bfloat16)
        return carry

    lax.fori_loop(0, rows, make_source, 0)
    chunks = depth // LANES
    sends_s = []
    for z in range(chunks):
        cols = pl.ds(z * LANES, LANES)
        sends_s.append([])
        for i in range(1, rows):
            copy = to_row(
                src.at[lax.rem(me + i, rows), :, :, cols], got_s.at[:, mine, cols],
                s_send.at[z, i], s_recv.at[z, i], i,
            )
            copy.start()
            sends_s[z].append(copy)
    own_s = pltpu.make_async_copy(src.at[me], got_s.at[:, mine, :], own_sem.at[1])
    own_s.start()

    tile = (RADIX, inner)
    k1s = lax.broadcasted_iota(jnp.int32, tile, 0)
    k2s = lax.broadcasted_iota(jnp.int32, tile, 1)
    modes = k1s + RADIX * k2s
    wave_x = jnp.where(modes >= total_x // 2, modes - total_x, modes).astype(f32) * (
        full_turn / total_x
    )
    wave_y = jnp.full(tile, plane[me], jnp.int32).astype(f32) * wave_unit
    wave_sq = wave_x * wave_x + wave_y * wave_y

    def width_at(j):
        return jnp.full(tile, spacing[level[jnp.clip(j, 0, total_z - 1)]], f32)

    def factor(j, carry):
        excess, h_prev, h_now, homog = carry
        at = base + j
        h_next = width_at(at + 1)
        flag_lo = jnp.where(at > 0, 1.0, 0.0).astype(f32)
        flag_hi = jnp.where(at < total_z - 1, 1.0, 0.0).astype(f32)
        lower = flag_lo / (0.5 * (h_prev + h_now) * h_now)
        upper = flag_hi / (0.5 * (h_now + h_next) * h_now)
        s = wave_sq + lower * excess
        q = 1.0 / (upper + s)
        homog = lower * q * homog
        rows_j = pl.ds(pl.multiple_of(j * RADIX, RADIX), RADIX)
        qq[rows_j, :] = q
        lq[rows_j, :] = lower * q
        uq[rows_j, :] = upper * q
        from_lo[rows_j, :] = homog
        return s * q, h_now, h_next, homog

    one = jnp.ones(tile, f32)
    lax.fori_loop(0, depth, factor, (one, width_at(base - 1), width_at(base), one), unroll=8)

    def factor_back(t, carry):
        lo, hi = carry
        j = depth - 1 - t
        rows_j = pl.ds(pl.multiple_of(j * RADIX, RADIX), RADIX)
        ratio = uq[rows_j, :]
        lo = from_lo[rows_j, :] + ratio * lo
        hi = ratio * hi
        from_lo[rows_j, :] = lo
        from_hi[rows_j, :] = hi
        return lo, hi

    lax.fori_loop(0, depth, factor_back, (jnp.zeros(tile, f32), one), unroll=16)
    top = (depth - 1) * RADIX
    coef[gz, 0] = from_lo[0:RADIX, :]
    coef[gz, 1] = from_hi[0:RADIX, :]
    coef[gz, 2] = from_lo[top : top + RADIX, :]
    coef[gz, 3] = from_hi[top : top + RADIX, :]
    sends_c = []
    for i in range(1, groups):
        copy = to_group(coef.at[gz], coef.at[gz], c_send.at[i], c_recv.at[i], i)
        copy.start()
        sends_c.append(copy)

    step = 16

    def first_stage(field, begin, end):
        def body(t, carry):
            at = pl.multiple_of(t * step, step)
            for lane in range(begin, end, LANES):
                cols = pl.ds(lane, LANES)
                re = [field[0, pl.ds(r * inner + at, step), cols].astype(f32) for r in range(RADIX)]
                im = [field[1, pl.ds(r * inner + at, step), cols].astype(f32) for r in range(RADIX)]
                re, im = radix_eight(re, im, -1.0)
                for k in range(RADIX):
                    h, l = split(re[k])
                    yh[k, pl.ds(at, step), cols] = h
                    yl[k, pl.ds(at, step), cols] = l
                    h, l = split(im[k])
                    yh[k, pl.ds(inner + at, step), cols] = h
                    yl[k, pl.ds(inner + at, step), cols] = l
            return carry

        lax.fori_loop(0, inner // step, body, 0, unroll=2)

    over_rows = (((0,), (0,)), ((), ()))
    over_last = (((1,), (1,)), ((), ()))

    def dot(a, b, dims):
        return lax.dot_general(a, b, dims, preferred_element_type=f32)

    def second_stage(combine, begin, end):
        cols = pl.ds(begin, end - begin)

        def body(k, carry):
            h, l, a, b = yh[k, :, cols], yl[k, :, cols], wh[k], wl[k]
            hat = dot(h, a, over_rows) + dot(h, b, over_rows) + dot(l, a, over_rows)
            where = pl.ds(begin * RADIX + k, end - begin, stride=RADIX)
            combine(k, where, hat[:, :inner], hat[:, inner:])
            return carry

        lax.fori_loop(0, RADIX, body, 0, unroll=4)

    def put_along(k, where, re, im):
        number = k + RADIX * lax.broadcasted_iota(jnp.int32, (1, inner), 1)
        column = jnp.where(number >= total_x // 2, number - total_x, number).astype(f32) * (
            full_turn / total_x
        )
        rhs_re[where, :] = -column * im
        rhs_im[where, :] = column * re

    def put_source(k, where, re, im):
        rhs_re[where, :] = rhs_re[where, :] + re
        rhs_im[where, :] = rhs_im[where, :] + im

    own_u.wait()
    for copy in sends_u:
        copy.wait_recv()
    for load in loads[2:]:
        load.wait()
    first_stage(got_u, 0, depth)
    second_stage(put_along, 0, depth)
    own_s.wait()
    for z in range(chunks):
        for copy in sends_s[z]:
            copy.wait_recv()
        first_stage(got_s, z * LANES, (z + 1) * LANES)
        second_stage(put_source, z * LANES, (z + 1) * LANES)

    def sweep(j, carry):
        re, im = carry
        rows_j = pl.ds(pl.multiple_of(j * RADIX, RADIX), RADIX)
        q, low = qq[rows_j, :], lq[rows_j, :]
        re = low * re - q * rhs_re[rows_j, :]
        im = low * im - q * rhs_im[rows_j, :]
        rhs_re[rows_j, :] = re
        rhs_im[rows_j, :] = im
        return re, im

    def sweep_back(t, carry):
        re, im = carry
        rows_j = pl.ds(pl.multiple_of((depth - 1 - t) * RADIX, RADIX), RADIX)
        ratio = uq[rows_j, :]
        re = rhs_re[rows_j, :] + ratio * re
        im = rhs_im[rows_j, :] + ratio * im
        rhs_re[rows_j, :] = re
        rhs_im[rows_j, :] = im
        return re, im

    zero = jnp.zeros(tile, f32)
    lax.fori_loop(0, depth, sweep, (zero, zero), unroll=16)
    lax.fori_loop(0, depth, sweep_back, (zero, zero), unroll=16)

    edge[gz, 0] = rhs_re[0:RADIX, :]
    edge[gz, 1] = rhs_re[top : top + RADIX, :]
    edge[gz, 2] = rhs_im[0:RADIX, :]
    edge[gz, 3] = rhs_im[top : top + RADIX, :]
    sends_e = []
    for i in range(1, groups):
        copy = to_group(edge.at[gz], edge.at[gz], e_send.at[i], e_recv.at[i], i)
        copy.start()
        sends_e.append(copy)
    for copy in sends_c + sends_e:
        copy.wait_recv()
    if True:
        last_const, last_ratio = [(zero, zero)], [zero]
        head_const, head_ratio = [], []
        for b in range(groups):
            a0, b0, a1, b1 = (coef[b, n] for n in range(4))
            inv = 1.0 / (1.0 - a0 * last_ratio[b])
            ratio = b0 * inv
            head_ratio.append(ratio)
            heads, lasts = [], []
            for part_of in range(2):
                prev = last_const[b][part_of]
                head = (edge[b, 2 * part_of] + a0 * prev) * inv
                heads.append(head)
                lasts.append(edge[b, 2 * part_of + 1] + a1 * (prev + last_ratio[b] * head))
            head_const.append(heads)
            last_const.append(lasts)
            last_ratio.append(a1 * last_ratio[b] * ratio + b1)
        for part_of in range(2):
            following = zero
            heads = [zero] * (groups + 1)
            for b in reversed(range(groups)):
                heads[b] = head_const[b][part_of] + head_ratio[b] * heads[b + 1]
            for b in range(groups):
                below = last_const[b][part_of] + last_ratio[b] * heads[b]
                solved[b, part_of, 0] = below
                solved[b, part_of, 1] = heads[b + 1]
    below_re, above_re = solved[gz, 0, 0], solved[gz, 0, 1]
    below_im, above_im = solved[gz, 1, 0], solved[gz, 1, 1]

    def join(j, carry):
        rows_j = pl.ds(pl.multiple_of(j * RADIX, RADIX), RADIX)
        lo, hi = from_lo[rows_j, :], from_hi[rows_j, :]
        rhs_re[rows_j, :] = rhs_re[rows_j, :] + lo * below_re + hi * above_re
        rhs_im[rows_j, :] = rhs_im[rows_j, :] + lo * below_im + hi * above_im
        return carry

    scale = 1.0 / total_x
    sends_p = []
    own_p = []
    for z in range(depth // LANES):
        start = z * LANES
        cols = pl.ds(start, LANES)
        lax.fori_loop(start, start + LANES, join, 0, unroll=16)

        def inverse(k, carry):
            where = pl.ds(start * RADIX + k, LANES, stride=RADIX)
            line = jnp.concatenate([rhs_re[where, :], rhs_im[where, :]], axis=1)
            h, l = split(line)
            a, b = wh[k], wl[k]
            spec[k] = dot(a, h, over_last) + dot(b, h, over_last) + dot(a, l, over_last)
            return carry

        lax.fori_loop(0, RADIX, inverse, 0, unroll=4)

        def last_stage(t, carry):
            at = pl.multiple_of(t * step, step)
            re = [spec[k, pl.ds(at, step), :] for k in range(RADIX)]
            im = [spec[k, pl.ds(inner + at, step), :] for k in range(RADIX)]
            re, im = radix_eight(re, im, 1.0)
            for r in range(RADIX):
                back[0, pl.ds(r * inner + at, step), cols] = (re[r] * scale).astype(jnp.bfloat16)
                back[1, pl.ds(r * inner + at, step), cols] = (im[r] * scale).astype(jnp.bfloat16)
            return carry

        lax.fori_loop(0, inner // step, last_stage, 0)
        for i in range(1, rows):
            theirs = pl.ds(pl.multiple_of(lax.rem(me + i, rows) * part, part), part)
            copy = to_row(
                back.at[:, theirs, cols], out.at[:, me, :, cols],
                p_send.at[z, i], p_recv.at[z, i], i,
            )
            copy.start()
            sends_p.append(copy)
        copy = pltpu.make_async_copy(
            back.at[:, mine, cols], out.at[:, me, :, cols], own_sem.at[2 + z]
        )
        copy.start()
        own_p.append(copy)
    for copy in sends_u + sum(sends_s, []) + sends_c + sends_e:
        copy.wait_send()
    for copy in own_p + sends_p:
        copy.wait()

    @pl.when(gz < groups - 1)
    def _():
        wall_copy.wait_send()


def on_device(rows, groups, velocity_x, velocity_y, velocity_z, spacing, level_index, plane_index):
    planes, part, depth = velocity_x.shape[1:]
    total_x = part * rows
    inner = total_x // RADIX
    assert planes == rows and depth % LANES == 0 and inner % LANES == 0
    high, low = phase_tables(total_x)
    bf16, f32 = jnp.bfloat16, jnp.float32
    vmem = pltpu.VMEM
    lines = (depth * RADIX, inner)
    dma = pltpu.SemaphoreType.DMA
    hbm = pl.BlockSpec(memory_space=pl.ANY)
    smem = pl.BlockSpec(memory_space=pltpu.SMEM)
    received = pl.pallas_call(
        functools.partial(kernel, rows, groups),
        out_shape=jax.ShapeDtypeStruct(velocity_x.shape, bf16),
        in_specs=[hbm] * 5 + [pl.BlockSpec(memory_space=pltpu.VMEM), smem, smem, smem],
        out_specs=hbm,
        scratch_shapes=[
            vmem(velocity_y.shape, bf16),
            vmem(velocity_z.shape, bf16),
            vmem(high.shape, bf16),
            vmem(high.shape, bf16),
            vmem((part, LANES), bf16),
            vmem((part, LANES), bf16),
            vmem((planes, 2, part, depth), bf16),
            vmem((2, total_x, depth), bf16),
            vmem((2, total_x, depth), bf16),
            vmem((RADIX, 2 * inner, depth), bf16),
            vmem((RADIX, 2 * inner, depth), bf16),
        ]
        + [vmem(lines, f32)] * 7
        + [
            vmem((groups, 4, RADIX, inner), f32),
            vmem((groups, 4, RADIX, inner), f32),
            vmem((groups, 2, 2, RADIX, inner), f32),
            vmem((RADIX, 2 * inner, LANES), f32),
            vmem((2, total_x, depth), bf16),
            dma((4,)),
            dma((2 + depth // LANES,)),
            dma((rows,)), dma((rows,)),
            dma((depth // LANES, rows)), dma((depth // LANES, rows)),
            dma, dma,
            dma((groups,)), dma((groups,)), dma((groups,)), dma((groups,)),
            dma((depth // LANES, rows)), dma((depth // LANES, rows)),
        ],
        compiler_params=pltpu.CompilerParams(
            collective_id=0, has_side_effects=True, vmem_limit_bytes=56 * 1024 * 1024
        ),
    )(
        velocity_x, velocity_y, velocity_z, jnp.asarray(high), jnp.asarray(low),
        level_index.reshape(1, -1), spacing, level_index, plane_index,
    )
    return received.astype(f32)


def solution(mesh):
    placed = (
        P(None, None, "row", "gz"),
        P(None, None, "row", "gz"),
        P(None, None, "row", "gz"),
        P(),
        P(),
        P(),
    )
    body = functools.partial(on_device, mesh.shape["row"], mesh.shape["gz"])
    return jax.shard_map(
        body, mesh=mesh, in_specs=placed, out_specs=P(None, None, "row", "gz"), check_vma=False
    )
```
